32 devices in a mesh: row: 8 (over y, x, core), col: 4 (over z).
Axes of the slice: x: 2, y: 2, z: 4, core: 2. Of those that a mesh axis runs over, the one named last changes fastest.
Arguments:
- vectors: float32 [32768, 4096], P('row', 'col'), may hold values from -6 to 6
- reflectors: float32 [8, 32768, 128], P('col', 'row'), may hold values from -0.03125 to 0.03125
- triangles: float32 [8, 128, 128], P('col'), may hold values from -0.25 to 1.8, as said below
Outputs:
- transformed: float32 [32768, 4096], P('row', 'col')
The draws below stay inside these ranges and needn't reach their ends.
Inputs may be any that keep to these rules, and one draw needn't show every extreme that they name: Each triangles[p] is upper triangular with diagonal entries between 0.5 and 1.8.
All inputs are finite; a program needn't handle non-finite values.
Results may differ from the reference program's by a relative error of at most 0.00013.
Values sent between devices are 32-bit elements; how exact they have to be, the bound alone decides.
A program may use at most 128 MiB of HBM per device.

```python
import jax
import jax.numpy as jnp
from jax import lax

ORDER = 32768
NB = 128
PANELS = 8
COLS = 4096


def draw_triangles(key, part):
    first, second = jax.random.split(jax.random.fold_in(key, 7))
    diagonal = jax.random.uniform(first, (PANELS, NB), jnp.float32, 0.5, 1.5)
    offdiag = jnp.clip(0.05 * jax.random.normal(second, (PANELS, NB, NB), jnp.float32), -0.25, 0.25)
    ident = jnp.eye(NB, dtype=jnp.float32)
    return jnp.triu(offdiag, 1) + diagonal[:, :, None] * ident[None, :, :]


def level_of(rng, shape, cuts, low, largest):
    def one(axis_at, shards_of):
        steps = jax.random.uniform(jax.random.fold_in(jax.random.fold_in(rng, 6), axis_at), (shards_of,), jnp.float32, low / len(cuts), largest / len(cuts))
        return jnp.repeat(jnp.exp(steps), shape[axis_at] // shards_of).reshape((-1,) + (1,) * (len(shape) - axis_at - 1))

    gain = one(*cuts[0])
    for cut in cuts[1:]:
        gain = gain * one(*cut)
    return gain


def noise(own_key, extent, scale, bound, shards=(), kind=jnp.bfloat16):
    result = scale * jax.random.normal(own_key, extent, jnp.float32)
    if shards:
        result = result * level_of(own_key, extent, shards, -0.22, 0.18)
    return jnp.clip(result, -bound, bound).astype(kind)


def setup_inputs(seed: int = 0) -> dict:
    key_list = jax.random.split(jax.random.key(seed), 4)
    vectors = noise(key_list[0], (ORDER, COLS), 1.0, 6.0, ((0, 8), (1, 4)), jnp.float32)
    reflectors = noise(key_list[1], (PANELS, ORDER, NB), ORDER ** -0.5, 0.03125, ((0, 4), (1, 8)), jnp.float32)
    triangles = draw_triangles(jax.random.fold_in(key_list[3], 71), 0)
    return dict(vectors=vectors, reflectors=reflectors, triangles=triangles)


def reference(vectors, reflectors, triangles):
    hi = lax.Precision.HIGHEST
    block = vectors
    for panel in range(PANELS - 1, -1, -1):
        basis = reflectors[panel]
        summed = lax.dot_general(basis, block, (((0,), (0,)), ((), ())), precision=hi, preferred_element_type=jnp.float32)
        scaled = jnp.dot(triangles[panel], summed, precision=hi, preferred_element_type=jnp.float32)
        block = block - jnp.dot(basis, scaled, precision=hi, preferred_element_type=jnp.float32)
    return block
```

```python
import jax
import jax.numpy as jnp
from jax import lax
from jax.sharding import PartitionSpec as P

FULL = lax.Precision.HIGHEST
THREE = lax.Precision.HIGH


def product_t(left, right, precision=THREE):
    return lax.dot_general(
        left,
        right,
        (((0,), (0,)), ((), ())),
        precision=precision,
        preferred_element_type=jnp.float32,
    )


def matmul(left, right, precision=THREE):
    return jnp.dot(left, right, precision=precision, preferred_element_type=jnp.float32)


def merge(tri_a, inner, tri_b):
    coupling = -matmul(matmul(tri_a, inner, FULL), tri_b, FULL)
    zero = jnp.zeros((tri_b.shape[0], tri_a.shape[1]), jnp.float32)
    return jnp.concatenate(
        [
            jnp.concatenate([tri_a, coupling], axis=1),
            jnp.concatenate([zero, tri_b], axis=1),
        ],
        axis=0,
    )


def after(value, earlier):
    return value + 0.0 * sum(array[0, 0] for array in earlier)


def ring_gather(panels, n):
    up = [(i, (i + 1) % n) for i in range(n)]
    down = [(i, (i - 1) % n) for i in range(n)]
    count = len(panels)
    near = {0: list(panels)}
    lower, upper = list(panels), list(panels)
    for step in range(1, (n - 1) // 2 + 1):
        lower = [lax.ppermute(lower[i], "col", up) for i in range(count)]
        upper = [lax.ppermute(upper[i], "col", down) for i in reversed(range(count))][::-1]
        near[n - step] = lower
        near[step] = upper
    if n % 2 == 0:
        half = (count + 1) // 2
        near[n // 2] = [lax.ppermute(lower[i], "col", up) for i in range(half)] + [
            lax.ppermute(upper[i], "col", down) for i in range(half, count)
        ]
    return near


def shards(vectors, reflectors, triangles):
    per_dev, _, nb = reflectors.shape
    n = lax.axis_size("col")
    rows = lax.axis_size("row")
    me = lax.axis_index("col")
    width = per_dev * nb

    near = ring_gather([reflectors[i] for i in range(per_dev)], n)
    basis = {r: jnp.concatenate(near[r], axis=1) for r in range(n)}

    summed = {}
    summed[0], inner = lax.psum((product_t(basis[0], vectors), product_t(basis[0], basis[0], FULL)), "row")
    tri = triangles[0]
    for i in range(1, per_dev):
        tri = merge(tri, inner[: i * nb, i * nb : (i + 1) * nb], triangles[i])

    last = n // 2
    pairs = []
    for d in range(1, n // 2 + 1):
        low, high = (-(d // 2)) % n, (d - d // 2) % n
        pairs.append(product_t(basis[low], basis[high], FULL))
    share = width // rows
    mine = [lax.dynamic_slice_in_dim(tri, lax.axis_index("row") * share, share, 0)]
    if pairs:
        split = lax.psum_scatter(jnp.stack(pairs), "row", scatter_dimension=1, tiled=True)
        mine += [split[i] for i in range(len(pairs))]
    shared = lax.all_gather(jnp.stack(mine), ("col", "row"), axis=0)
    shared = shared.reshape(n, rows, len(mine), share, width)
    shared = shared.transpose(0, 2, 1, 3, 4).reshape(n, len(mine), width, width)

    def inner_of(i, j):
        ahead = j - i
        d = min(ahead, n - ahead)
        if ahead == d:
            return shared[(i + d // 2) % n, d]
        return shared[(j + d // 2) % n, d].T

    tris = [(i, i + 1, shared[i, 0]) for i in range(n)]
    while len(tris) > 1:
        merged = []
        for a, b in zip(tris[::2], tris[1::2]):
            inner_ab = jnp.concatenate(
                [jnp.concatenate([inner_of(i, j) for j in range(b[0], b[1])], axis=1) for i in range(a[0], a[1])],
                axis=0,
            )
            merged.append((a[0], b[1], merge(a[2], inner_ab, b[2])))
        if len(tris) % 2:
            merged.append(tris[-1])
        tris = merged
    whole = tris[0][2].reshape(n, width, n, width)
    whole = lax.dynamic_slice_in_dim(jnp.concatenate([whole, whole], axis=0), me, n, 0)
    whole = whole.transpose(2, 0, 1, 3)
    whole = lax.dynamic_slice_in_dim(jnp.concatenate([whole, whole], axis=0), me, n, 0)
    columns = [whole[r].reshape(n * width, width) for r in range(n)]

    early = [r for r in range(1, n) if r != last]
    if early:
        joined = product_t(jnp.concatenate([basis[r] for r in early], axis=1), vectors)
        joined = lax.psum(after(joined, [summed[0], inner] + pairs), "row")
        for at, r in enumerate(early):
            summed[r] = joined[at * width : (at + 1) * width]
    order = [0] + early
    scaled = matmul(
        jnp.concatenate([columns[r] for r in order], axis=1),
        jnp.concatenate([summed[r] for r in order], axis=0),
    )
    if n > 1:
        done = [summed[early[-1]] if early else summed[0]]
        summed[last] = lax.psum(after(product_t(basis[last], vectors), done), "row")
        scaled = scaled + matmul(columns[last], summed[last])
    return vectors - matmul(jnp.concatenate([basis[r] for r in range(n)], axis=1), scaled)


def solution(mesh):
    placed = (P("row", "col"), P("col", "row", None), P("col", None, None))
    return jax.shard_map(
        shards, mesh=mesh, in_specs=placed, out_specs=P("row", "col"), check_vma=False
    )
```
